32 devices in a mesh: fsdp: 32 (over z, y, x, core).
Axes of the slice: x: 2, y: 2, z: 4, core: 2. Of those that a mesh axis runs over, the one named last changes fastest.
Arguments:
- token_ids: int32 [32, 512], P('fsdp')
- grad_y: bfloat16 [32, 512, 896], P('fsdp')
- table: bfloat16 [151936, 896], P('fsdp')
- norm1_gain: bfloat16 [896], P('fsdp')
- norm2_gain: bfloat16 [896], P('fsdp')
- w_query: bfloat16 [896, 14, 64], P('fsdp')
- w_key: bfloat16 [896, 2, 64], P('fsdp')
- w_value: bfloat16 [896, 2, 64], P('fsdp')
- w_out: bfloat16 [896, 896], P('fsdp')
- w_gate: bfloat16 [896, 4864], P('fsdp')
- w_up: bfloat16 [896, 4864], P('fsdp')
- w_down: bfloat16 [4864, 896], P('fsdp')
Outputs:
- output 1: bfloat16 [32, 512, 896], P('fsdp')
- output 2: bfloat16 [151936, 896], P('fsdp')
- output 3: bfloat16 [896], P('fsdp')
- output 4: bfloat16 [896], P('fsdp')
- output 5: bfloat16 [896, 14, 64], P('fsdp')
- output 6: bfloat16 [896, 2, 64], P('fsdp')
- output 7: bfloat16 [896, 2, 64], P('fsdp')
- output 8: bfloat16 [896, 896], P('fsdp')
- output 9: bfloat16 [896, 4864], P('fsdp')
- output 10: bfloat16 [896, 4864], P('fsdp')
- output 11: bfloat16 [4864, 896], P('fsdp')
All inputs are finite; a program needn't handle non-finite values.
Results may differ from the reference program's by a relative error of at most 0.0156545.
Values are sent between devices in bfloat16 or wider.
A program may use at most 1 GiB of HBM per device.

```python
import jax
import jax.numpy as jnp
from jax import lax

VOCAB_SIZE = 151936
MODEL_DIM = 896
Q_HEADS = 14
KV_HEADS = 2
HEAD_DIM = 64
FFN_DIM = 4864
GLOBAL_BATCH = 32
SEQ_LEN = 512

NORM_EPS = 1e-5
ROPE_THETA = 500000.0
VOCAB_BITS = (VOCAB_SIZE - 1).bit_length()
TOKENS_ALL = GLOBAL_BATCH * SEQ_LEN


def draw_ids(rng_key):
    k_level, k_rank, k_flat, k_pick, k_perm = jax.random.split(rng_key, 5)
    id_shape = (GLOBAL_BATCH, SEQ_LEN)
    levels = jax.random.randint(k_level, id_shape, 0, VOCAB_BITS + 1)
    level_span = jnp.minimum(jnp.left_shift(jnp.ones(id_shape, jnp.int32), levels), VOCAB_SIZE)
    id_ranks = jax.random.randint(k_rank, id_shape, 0, level_span)
    flat_ids = jax.random.randint(k_flat, id_shape, 0, VOCAB_SIZE)
    use_flat = jax.random.randint(k_pick, id_shape, 0, 4) == 0
    id_ranks = jnp.where(use_flat, flat_ids, id_ranks)
    row_order = jax.random.permutation(k_perm, VOCAB_SIZE)
    return jnp.take(row_order, id_ranks).astype(jnp.int32)


def normal_weight(rng_key, w_shape, fan_in):
    return (jax.random.normal(rng_key, w_shape, jnp.float32) * fan_in ** -0.5).astype(jnp.bfloat16)


def setup_inputs(seed: int = 0) -> dict:
    keys = jax.random.split(jax.random.key(seed), 12)
    attn_width = Q_HEADS * HEAD_DIM
    return {
        "token_ids": draw_ids(keys[0]),
        "grad_y": (jax.random.normal(keys[1], (GLOBAL_BATCH, SEQ_LEN, MODEL_DIM), jnp.float32) * TOKENS_ALL ** -0.5).astype(jnp.bfloat16),
        "table": jax.random.normal(keys[2], (VOCAB_SIZE, MODEL_DIM), jnp.float32).astype(jnp.bfloat16),
        "norm1_gain": jax.random.uniform(keys[3], (MODEL_DIM,), jnp.float32, 0.5, 1.5).astype(jnp.bfloat16),
        "norm2_gain": jax.random.uniform(keys[4], (MODEL_DIM,), jnp.float32, 0.5, 1.5).astype(jnp.bfloat16),
        "w_query": normal_weight(keys[5], (MODEL_DIM, Q_HEADS, HEAD_DIM), MODEL_DIM),
        "w_key": normal_weight(keys[6], (MODEL_DIM, KV_HEADS, HEAD_DIM), MODEL_DIM),
        "w_value": normal_weight(keys[7], (MODEL_DIM, KV_HEADS, HEAD_DIM), MODEL_DIM),
        "w_out": normal_weight(keys[8], (attn_width, MODEL_DIM), attn_width),
        "w_gate": normal_weight(keys[9], (MODEL_DIM, FFN_DIM), MODEL_DIM),
        "w_up": normal_weight(keys[10], (MODEL_DIM, FFN_DIM), MODEL_DIM),
        "w_down": normal_weight(keys[11], (FFN_DIM, MODEL_DIM), FFN_DIM),
    }


def rms_norm(x_f32, gain_f32):
    inv_rms = lax.rsqrt(jnp.mean(x_f32 * x_f32, axis=-1, keepdims=True) + NORM_EPS)
    return (x_f32 * inv_rms * gain_f32).astype(jnp.bfloat16)


def rotary(x_f32):
    head_dim = x_f32.shape[-1]
    half_dim = head_dim // 2
    seq_len = x_f32.shape[-3]
    inv_freq = ROPE_THETA ** (-2.0 * jnp.arange(half_dim, dtype=jnp.float32) / head_dim)
    angles = jnp.arange(seq_len, dtype=jnp.float32)[:, None] * inv_freq[None, :]
    cos_tab = jnp.cos(angles)[:, None, :]
    sin_tab = jnp.sin(angles)[:, None, :]
    lo_half = x_f32[..., :half_dim]
    hi_half = x_f32[..., half_dim:]
    return jnp.concatenate([lo_half * cos_tab - hi_half * sin_tab, hi_half * cos_tab + lo_half * sin_tab], axis=-1)


def attend(q_f32, k_f32, v_bf16):
    q_rot = rotary(q_f32).astype(jnp.bfloat16).reshape(SEQ_LEN, KV_HEADS, Q_HEADS // KV_HEADS, HEAD_DIM)
    k_rot = rotary(k_f32).astype(jnp.bfloat16)
    scores = jnp.einsum("qkgd,skd->kgqs", q_rot.astype(jnp.float32), k_rot.astype(jnp.float32)) * HEAD_DIM ** -0.5
    positions = jnp.arange(SEQ_LEN)
    causal = positions[:, None] >= positions[None, :]
    scores = jnp.where(causal, scores, -1e30)
    prob_bf = jax.nn.softmax(scores, axis=-1).astype(jnp.bfloat16)
    attn_out = jnp.einsum("kgqs,skd->qkgd", prob_bf.astype(jnp.float32), v_bf16.astype(jnp.float32))
    return attn_out.astype(jnp.bfloat16).reshape(SEQ_LEN, Q_HEADS * HEAD_DIM)


def layer(emb_rows, gain_one, gain_two, w_query, w_key, w_value, w_out, w_gate, w_up, w_down):
    x_f32 = emb_rows.astype(jnp.float32)
    h_one = rms_norm(x_f32, gain_one).astype(jnp.float32)
    q_f32 = jnp.einsum("sd,dhe->she", h_one, w_query)
    k_f32 = jnp.einsum("sd,dhe->she", h_one, w_key)
    v_bf16 = jnp.einsum("sd,dhe->she", h_one, w_value).astype(jnp.bfloat16)
    attn_out = attend(q_f32, k_f32, v_bf16)
    resid_f32 = x_f32 + jnp.dot(attn_out.astype(jnp.float32), w_out, preferred_element_type=jnp.float32)
    resid_two = resid_f32.astype(jnp.bfloat16).astype(jnp.float32)
    h_two = rms_norm(resid_two, gain_two).astype(jnp.float32)
    gate_f32 = jnp.dot(h_two, w_gate, preferred_element_type=jnp.float32)
    up_f32 = jnp.dot(h_two, w_up, preferred_element_type=jnp.float32)
    act_f32 = (jax.nn.silu(gate_f32) * up_f32).astype(jnp.bfloat16).astype(jnp.float32)
    return (resid_two + jnp.dot(act_f32, w_down, preferred_element_type=jnp.float32)).astype(jnp.bfloat16)


def reference(token_ids, grad_y, table, norm1_gain, norm2_gain, w_query, w_key, w_value, w_out, w_gate, w_up, w_down):
    params = tuple(weight.astype(jnp.float32) for weight in (norm1_gain, norm2_gain, w_query, w_key, w_value, w_out, w_gate, w_up, w_down))

    def one_sequence(grad_acc, seq_in):
        seq_ids, seq_dy = seq_in
        emb_rows = jnp.take(table, seq_ids, axis=0)
        layer_out, pullback = jax.vjp(layer, emb_rows, *params)
        cotangents = pullback(seq_dy)
        new_acc = tuple(acc_old + cot_new for acc_old, cot_new in zip(grad_acc, cotangents[1:]))
        return new_acc, (layer_out, cotangents[0])

    zero_acc = tuple(jnp.zeros_like(weight) for weight in params)
    grad_acc, (y_out, d_emb) = lax.scan(one_sequence, zero_acc, (token_ids, grad_y))
    grad_table = jax.ops.segment_sum(d_emb.reshape(-1, MODEL_DIM).astype(jnp.float32), token_ids.reshape(-1), num_segments=VOCAB_SIZE).astype(jnp.bfloat16)
    grads = [acc_val.astype(jnp.bfloat16) for acc_val in grad_acc]
    return (y_out, grad_table, grads[0], grads[1], grads[2], grads[3], grads[4], grads[5], grads[6], grads[7], grads[8])
```

```python
import jax
import jax.numpy as jnp
from jax import lax
from jax.sharding import PartitionSpec as P

AXIS_NAME = "fsdp"
NORM_EPS = 1e-5
ROPE_THETA = 500000.0
SLOTS = 32


def rms_norm(x_f32, gain_f32):
    inv_rms = lax.rsqrt(jnp.mean(x_f32 * x_f32, axis=-1, keepdims=True) + NORM_EPS)
    return (x_f32 * inv_rms * gain_f32).astype(jnp.bfloat16)


def rotary(x_f32):
    head_dim = x_f32.shape[-1]
    half_dim = head_dim // 2
    seq_len = x_f32.shape[-3]
    inv_freq = ROPE_THETA ** (-2.0 * jnp.arange(half_dim, dtype=jnp.float32) / head_dim)
    angles = jnp.arange(seq_len, dtype=jnp.float32)[:, None] * inv_freq[None, :]
    cos_tab = jnp.cos(angles)[:, None, :]
    sin_tab = jnp.sin(angles)[:, None, :]
    lo_half = x_f32[..., :half_dim]
    hi_half = x_f32[..., half_dim:]
    return jnp.concatenate([lo_half * cos_tab - hi_half * sin_tab, hi_half * cos_tab + lo_half * sin_tab], axis=-1)


def attend(q_f32, k_f32, v_bf16):
    batch_loc, seq_len, q_heads, head_dim = q_f32.shape
    kv_heads = k_f32.shape[2]
    q_rot = rotary(q_f32).astype(jnp.bfloat16).reshape(batch_loc, seq_len, kv_heads, q_heads // kv_heads, head_dim)
    k_rot = rotary(k_f32).astype(jnp.bfloat16)
    scores = jnp.einsum("bqkgd,bskd->bkgqs", q_rot, k_rot, preferred_element_type=jnp.float32) * head_dim ** -0.5
    positions = jnp.arange(seq_len)
    causal = positions[:, None] >= positions[None, :]
    scores = jnp.where(causal, scores, -1e30)
    prob_bf = jax.nn.softmax(scores, axis=-1).astype(jnp.bfloat16)
    attn_out = jnp.einsum("bkgqs,bskd->bqkgd", prob_bf, v_bf16, preferred_element_type=jnp.float32)
    return attn_out.astype(jnp.bfloat16).reshape(batch_loc, seq_len, q_heads * head_dim)


def gated(gate_f32, up_f32):
    return (jax.nn.silu(gate_f32) * up_f32).astype(jnp.bfloat16)


def matmul(lhs, rhs):
    return jnp.dot(lhs, rhs, preferred_element_type=jnp.float32)


def matmul_nt(lhs, rhs):
    return lax.dot_general(lhs, rhs, (((1,), (1,)), ((), ())), preferred_element_type=jnp.float32)


def matmul_tn(lhs, rhs):
    return lax.dot_general(lhs, rhs, (((0,), (0,)), ((), ())), preferred_element_type=jnp.float32)


BIT_CORE, BIT_X, BIT_Y, BIT_ZLO, BIT_ZHI = 0, 1, 2, 3, 4
AXIS_OF_BIT = {BIT_ZHI: 0, BIT_ZLO: 1, BIT_Y: 2, BIT_X: 3}
ORDER_A = (BIT_ZHI, BIT_ZLO, BIT_Y, BIT_X)
ORDER_B = (BIT_ZHI, BIT_ZLO, BIT_X, BIT_Y)
ORDER_C = (BIT_Y, BIT_X, BIT_ZHI, BIT_ZLO)
DOWN_CUT = 80


def solution(mesh):
    n_dev = mesh.shape[AXIS_NAME]
    chips = n_dev // 2
    spec_1d = P(AXIS_NAME)
    spec_2d = P(AXIS_NAME, None)
    spec_3d = P(AXIS_NAME, None, None)
    in_specs = (spec_2d, spec_3d, spec_2d, spec_1d, spec_1d, spec_3d, spec_3d, spec_3d, spec_2d, spec_2d, spec_2d, spec_2d)
    out_specs = (spec_3d, spec_2d, spec_1d, spec_1d, spec_3d, spec_3d, spec_3d, spec_2d, spec_2d, spec_2d, spec_2d)

    def swap(val, bit):
        return lax.ppermute(val, AXIS_NAME, [(i, i ^ (1 << bit)) for i in range(n_dev)])

    def my_bit(bit):
        return (lax.axis_index(AXIS_NAME) >> bit) & 1

    def gather_chips(block, order):
        buf = block[None, None, None, None]
        for bit in order:
            axis = AXIS_OF_BIT[bit]
            got = swap(buf, bit)
            buf = jnp.where(my_bit(bit) == 0, jnp.concatenate([buf, got], axis=axis), jnp.concatenate([got, buf], axis=axis))
        return buf.reshape((chips,) + block.shape)

    def scatter_chips(grad, order):
        buf = grad.reshape((2, 2, 2, 2) + grad.shape[1:])
        for bit in reversed(order):
            axis = AXIS_OF_BIT[bit]
            mine = my_bit(bit)
            send = lax.dynamic_index_in_dim(buf, 1 - mine, axis, keepdims=True)
            keep = lax.dynamic_index_in_dim(buf, mine, axis, keepdims=True)
            buf = keep + swap(send, bit)
        return buf.reshape(grad.shape[1:])

    def by_core(mine, other):
        is_zero = my_bit(BIT_CORE) == 0
        return jnp.where(is_zero, mine, other), jnp.where(is_zero, other, mine)

    def pick_core(of_zero, of_one):
        is_zero = my_bit(BIT_CORE) == 0
        return jnp.where(is_zero, of_zero, of_one), jnp.where(is_zero, of_one, of_zero)

    def device_step(token_ids, grad_y, table, norm1_gain, norm2_gain, w_query, w_key, w_value, w_out, w_gate, w_up, w_down):
        me = lax.axis_index(AXIS_NAME)
        rows_dev, dim = table.shape
        seq_len = token_ids.shape[1]
        d_loc = w_out.shape[0]
        ffn = w_gate.shape[1]
        f_loc = w_down.shape[0]
        q_heads, head_dim = w_query.shape[1:]
        kv_heads = w_key.shape[1]
        kv_dim = kv_heads * head_dim

        gains = jnp.pad(jnp.stack([norm1_gain, norm2_gain], axis=1), ((0, 0), (0, 126)))
        set_zero = jnp.concatenate([w_query.reshape(d_loc, dim), w_key.reshape(d_loc, kv_dim), gains], axis=1)
        set_one = jnp.concatenate([w_out, w_value.reshape(d_loc, kv_dim), gains], axis=1)

        def ffn_halves(w_shard):
            halves = w_shard.reshape(d_loc, chips, 2, f_loc)
            return halves[:, :, 0].reshape(d_loc, ffn // 2), halves[:, :, 1].reshape(d_loc, ffn // 2)

        gate_zero, gate_one = ffn_halves(w_gate)
        up_zero, up_one = ffn_halves(w_up)
        mine, other = pick_core(
            jnp.concatenate([set_zero, gate_zero, up_zero], axis=1), jnp.concatenate([set_one, gate_one, up_one], axis=1)
        )
        chip_block = jnp.concatenate(by_core(mine, swap(other, BIT_CORE)), axis=0)
        attn_cols = set_zero.shape[1]
        half_cols = ffn // 2
        attn_block = chip_block[:, :attn_cols]
        gate_block = chip_block[:, attn_cols : attn_cols + half_cols]
        up_block = chip_block[:, attn_cols + half_cols :]
        attn_mine = gather_chips(attn_block, ORDER_C).reshape(dim, attn_cols)
        gate_w = gather_chips(gate_block, ORDER_A).reshape(dim, half_cols)
        up_w = gather_chips(up_block, ORDER_B).reshape(dim, half_cols)
        down_parts = [gather_chips(w_down[:DOWN_CUT], ORDER_A), gather_chips(w_down[DOWN_CUT:], ORDER_B)]
        down_w = jnp.concatenate(down_parts, axis=1).reshape(half_cols, dim)
        attn_zero, attn_one = by_core(attn_mine, swap(attn_mine, BIT_CORE))
        wq, wk = attn_zero[:, :dim], attn_zero[:, dim : dim + kv_dim]
        wo, wv = attn_one[:, :dim], attn_one[:, dim : dim + kv_dim]
        gain_cols = attn_zero[:, dim + kv_dim :].astype(jnp.float32)
        gain_one, gain_two = gain_cols[:, 0], gain_cols[:, 1]
        dy_own = grad_y[0]
        dy_pair = jnp.concatenate([dy_own, swap(dy_own, BIT_CORE)], axis=0)

        ids = token_ids[0]
        owner = ids // rows_dev
        local = ids - owner * rows_dev
        pos = jnp.arange(seq_len)
        same_id = ids[:, None] == ids[None, :]
        before = pos[None, :] < pos[:, None]
        first = jnp.logical_not(jnp.any(same_id & before, axis=1))
        rank = jnp.sum(((owner[:, None] == owner[None, :]) & before & first[None, :]).astype(jnp.int32), axis=1)
        slot = jnp.sum(jnp.where(same_id & first[None, :], rank[None, :], 0), axis=1)

        def hits(cap):
            place = jnp.where(slot < cap, owner * cap + slot, n_dev * cap)
            return jnp.arange(n_dev * cap)[:, None] == place[None, :]

        def wanted_rows(hit):
            return jnp.sum(jnp.where(hit & first[None, :], local[None, :] + 1, 0), axis=1) - 1

        def trade(val):
            return lax.all_to_all(val, AXIS_NAME, 0, 0, tiled=True)

        def fetch_rows(tab, asked, cap):
            picked = jnp.take(tab, jnp.maximum(asked, 0).reshape(-1), axis=0, mode="clip").reshape(n_dev, cap, dim)
            return jnp.take(trade(picked).reshape(n_dev * cap, dim), owner * cap + slot, axis=0, mode="clip")

        def send_sums(d_rows_loc, hit, cap):
            return trade(matmul(hit.astype(jnp.bfloat16), d_rows_loc).reshape(n_dev, cap, dim))

        def add_rows(got, asked):
            target = jnp.where(asked >= 0, asked, rows_dev).reshape(-1)
            return jax.ops.segment_sum(got.reshape(-1, dim), target, num_segments=rows_dev).astype(jnp.bfloat16)

        hit = hits(SLOTS)
        full = jnp.broadcast_to((jnp.max(slot) >= SLOTS).astype(jnp.int32), (n_dev, 128 - SLOTS))
        notes = trade(jnp.concatenate([wanted_rows(hit).reshape(n_dev, SLOTS), full], axis=1))
        asked = notes[:, :SLOTS]
        overflow = jnp.max(notes[:, SLOTS:]) > 0

        def rows_dense(_):
            asked_all = trade(wanted_rows(hits(seq_len)).reshape(n_dev, seq_len))
            return fetch_rows(table, asked_all, seq_len)

        emb_rows = lax.cond(overflow, rows_dense, lambda rows: rows, fetch_rows(table, asked, SLOTS))

        x_f32 = emb_rows.astype(jnp.float32)
        h_one, norm1_pull = jax.vjp(rms_norm, x_f32, gain_one)
        q_f32 = matmul(h_one, wq).reshape(1, seq_len, q_heads, head_dim)
        k_f32 = matmul(h_one, wk).reshape(1, seq_len, kv_heads, head_dim)
        v_bf16 = matmul(h_one, wv).astype(jnp.bfloat16).reshape(1, seq_len, kv_heads, head_dim)
        attn_out, attn_pull = jax.vjp(attend, q_f32, k_f32, v_bf16)
        attn_out = attn_out[0]
        resid_two = (x_f32 + matmul(attn_out, wo)).astype(jnp.bfloat16).astype(jnp.float32)
        h_two, norm2_pull = jax.vjp(rms_norm, resid_two, gain_two)

        h_pair = jnp.concatenate([h_two, swap(h_two, BIT_CORE)], axis=0)
        gate_f32 = matmul(h_pair, gate_w)
        up_f32 = matmul(h_pair, up_w)
        act_bf16, act_pull = jax.vjp(gated, gate_f32, up_f32)
        g_down = matmul_tn(act_bf16, dy_pair)
        g_down, dy_late = lax.optimization_barrier((g_down, dy_pair))
        d_act = matmul_nt(dy_late, down_w).astype(jnp.bfloat16)
        d_gate, d_up = act_pull(d_act)
        d_gate = d_gate.astype(jnp.bfloat16)
        d_up = d_up.astype(jnp.bfloat16)
        g_gate = matmul_tn(h_pair, d_gate)
        g_up = matmul_tn(h_pair, d_up)
        d_h_part = matmul_nt(d_gate, gate_w) + matmul_nt(d_up, up_w)
        act_late, d_h_part = lax.optimization_barrier((act_bf16, d_h_part))
        d_h_two = (d_h_part[:seq_len] + swap(d_h_part[seq_len:], BIT_CORE)).astype(jnp.bfloat16)
        y_part = matmul(act_late, down_w)
        layer_out = (resid_two + (y_part[:seq_len] + swap(y_part[seq_len:], BIT_CORE))).astype(jnp.bfloat16)

        g_down = g_down.reshape(chips, f_loc, dim)
        s_down = jnp.concatenate([scatter_chips(g_down[:, :DOWN_CUT], ORDER_A), scatter_chips(g_down[:, DOWN_CUT:], ORDER_B)], axis=0)
        s_gate = scatter_chips(g_gate.reshape(chips, 2 * d_loc, half_cols), ORDER_A)
        s_up = scatter_chips(g_up.reshape(chips, 2 * d_loc, half_cols), ORDER_B)

        d_resid_two, g_norm2 = norm2_pull(d_h_two)
        d_resid = (dy_own.astype(jnp.float32) + d_resid_two).astype(jnp.bfloat16)
        g_out = matmul_tn(attn_out, d_resid)
        d_attn = matmul_nt(d_resid, wo).astype(jnp.bfloat16)
        d_query, d_key, d_value = attn_pull(d_attn[None])
        d_query = d_query.astype(jnp.bfloat16).reshape(seq_len, dim)
        d_key = d_key.astype(jnp.bfloat16).reshape(seq_len, kv_dim)
        d_value = d_value.reshape(seq_len, kv_dim)
        d_h_one = (matmul_nt(d_query, wq) + matmul_nt(d_key, wk) + matmul_nt(d_value, wv)).astype(jnp.bfloat16)
        d_x, g_norm1 = norm1_pull(d_h_one)
        d_emb = (d_resid.astype(jnp.float32) + d_x).astype(jnp.bfloat16)

        def grads_dense(_):
            hit_all = hits(seq_len)
            asked_all = trade(wanted_rows(hit_all).reshape(n_dev, seq_len))
            return add_rows(send_sums(d_emb, hit_all, seq_len), asked_all)

        d_table = lax.cond(overflow, grads_dense, lambda got: add_rows(got, asked), send_sums(d_emb, hit, SLOTS))

        g_query = matmul_tn(h_one, d_query)
        g_key = matmul_tn(h_one, d_key)
        g_value = matmul_tn(h_one, d_value)
        g_gains = jnp.pad(jnp.stack([g_norm1, g_norm2], axis=1), ((0, 0), (0, 126)))
        keep, send = pick_core(
            jnp.concatenate([g_query, g_key, g_gains], axis=1), jnp.concatenate([g_out, g_value, jnp.zeros_like(g_gains)], axis=1)
        )
        attn_grad = (keep + swap(send, BIT_CORE)).reshape(chips, 2 * d_loc, attn_cols)
        s_attn = scatter_chips(attn_grad, ORDER_C)

        sums = jnp.concatenate([s_attn, s_gate, s_up], axis=1).astype(jnp.bfloat16)
        rows_mine, rows_other = pick_core(sums[:d_loc], sums[d_loc:])
        from_zero, from_one = by_core(rows_mine, swap(rows_other, BIT_CORE))

        def ffn_join(lo):
            parts = [part[:, lo : lo + half_cols].reshape(d_loc, chips, f_loc) for part in (from_zero, from_one)]
            return jnp.stack(parts, axis=2).reshape(d_loc, ffn)

        return (
            layer_out[None],
            d_table,
            from_zero[:, dim + kv_dim],
            from_zero[:, dim + kv_dim + 1],
            from_zero[:, :dim].reshape(w_query.shape),
            from_zero[:, dim : dim + kv_dim].reshape(w_key.shape),
            from_one[:, dim : dim + kv_dim].reshape(w_value.shape),
            from_one[:, :dim],
            ffn_join(attn_cols),
            ffn_join(attn_cols + half_cols),
            s_down.astype(jnp.bfloat16),
        )

    return jax.shard_map(device_step, mesh=mesh, in_specs=in_specs, out_specs=out_specs, check_vma=False)
```
